128 devices in a mesh: depth: 8 (over y, core), lat: 16 (over z, x).
Axes of the slice: x: 4, y: 4, z: 4, core: 2. Of those that a mesh axis runs over, the one named last changes fastest.
Arguments:
- emission: float32 [1024, 16, 2048], P('depth', None, 'lat'), may hold values from 0 to 2
- absorption: float32 [1024, 16, 2048], P('depth', None, 'lat'), may hold values from -4 to 4
- target: float32 [3, 16, 2048], P(None, None, 'lat'), may hold values from 0.2 to 0.8
- shift_whole: int32 [3, 1024], P(None, 'depth'), may hold values from -30 to 30, as said below
- shift_fraction: int32 [3, 1024], P(None, 'depth'), may hold values from 0 to 7, as said below
- taps_table: float32 [8, 4], replicated, may hold values from 0.05 to 0.45
Outputs:
- fitted_emission: float32 [1024, 16, 2048], P('depth', None, 'lat')
- fitted_absorption: float32 [1024, 16, 2048], P('depth', None, 'lat')
The draws below stay inside these ranges and needn't reach their ends.
Inputs may be any that keep to these rules, and one draw needn't show every extreme that they name: `shift_whole`: both ends of the range are taken in every draw. `shift_fraction`: every value of the range is taken in every draw.
All inputs are finite; a program needn't handle non-finite values.
Results may differ from the reference program's by a relative error of at most 0.0003.
Values sent between devices are 32-bit elements; how exact they have to be, the bound alone decides.
No kernel may reach another device: no remote copies, remote signals or barrier semaphores. Data moves between devices by JAX's collectives and lax.ppermute only.
A program may use at most 128 MiB of HBM per device.

```python
import jax
import jax.numpy as jnp
from jax import lax

R = 16
REACH = 32
TAPS = 4
FRACS = 8
ITERS = 3
NZ = 1024
NX = 2048


def shear_pair(key):
    key = jax.random.fold_in(key, 17)
    extreme = FRACS * (REACH - 2)
    key_size, key_sign, key_jitter = jax.random.split(key, 3)
    size_draw = jax.random.randint(key_size, (ITERS,), extreme // 2, extreme + 1, dtype=jnp.int32)
    direction_sign = 2 * jax.random.randint(key_sign, (ITERS,), 0, 2, dtype=jnp.int32) - 1
    views = jnp.arange(ITERS, dtype=jnp.int32)
    steepness = direction_sign * jnp.where(views == 0, extreme, size_draw)
    plane_index = jnp.arange(NZ, dtype=jnp.int32)
    eighths = steepness[:, None] * (2 * plane_index[None, :] - NZ + 1) // (NZ - 1)
    jitter = jax.random.randint(key_jitter, (ITERS, NZ), -1, 2, dtype=jnp.int32)
    interior = (plane_index > 0) & (plane_index < NZ - 1)
    eighths = jnp.clip(eighths + jnp.where(interior[None, :], jitter, 0), -extreme, extreme)
    eighths = jnp.where((views[:, None] == 0) & (plane_index[None, :] == 1), -1, eighths)
    return ((eighths // FRACS).astype(jnp.int32), (eighths % FRACS).astype(jnp.int32))


def draw_shift_whole(key, part):
    return shear_pair(key)[0]


def draw_shift_fraction(key, part):
    return shear_pair(key)[1]


def block_scale(key, shape, cuts, smallest, high):
    gain = 1.0
    for dim, blocks in cuts:
        draws = jax.random.uniform(jax.random.fold_in(jax.random.fold_in(key, 6), dim), (blocks,), jnp.float32, smallest / len(cuts), high / len(cuts))
        gain = gain * jnp.repeat(jnp.exp(draws), shape[dim] // blocks).reshape((-1,) + (1,) * (len(shape) - 1 - dim))
    return gain


def bell_draw(key, dims, width, reach, shards=(), kind=jnp.bfloat16):
    loudness = block_scale(key, dims, shards, -0.22, 0.18) if shards else 1.0
    result = jax.random.normal(key, dims, jnp.float32) * width * loudness
    return jnp.minimum(jnp.maximum(result, -reach), reach).astype(kind)


def setup_inputs(seed: int = 0) -> dict:
    arg_keys = jax.random.split(jax.random.key(seed), 7)
    return {
        "emission": jnp.clip(2.0 * jax.random.uniform(arg_keys[0], (NZ, R, NX), jnp.float32) ** block_scale(arg_keys[0], (NZ, R, NX), ((0, 8), (2, 16)), -0.2, 0.2), 0.0, 2.0),
        "absorption": bell_draw(arg_keys[1], (NZ, R, NX), 1.0, 4.0, ((0, 8), (2, 16)), jnp.float32),
        "target": jnp.clip(0.2 + 0.6 * jax.random.uniform(arg_keys[2], (ITERS, R, NX), jnp.float32) ** block_scale(arg_keys[2], (ITERS, R, NX), ((2, 16),), -0.2, 0.2), 0.2, 0.8),
        "shift_whole": draw_shift_whole(jax.random.fold_in(arg_keys[6], 71), 0),
        "shift_fraction": draw_shift_fraction(jax.random.fold_in(arg_keys[6], 71), 0),
        "taps_table": jnp.clip(jax.random.uniform(arg_keys[5], (FRACS, TAPS), jnp.float32, 0.05, 0.45), 0.05, 0.45),
    }


HIGHEST = lax.Precision.HIGHEST
LEARN_RATE = 0.1
BETA_FIRST = 0.9
BETA_SECOND = 0.999
ADAM_EPSILON = 0.001

def plane_taps(fractions, taps_table):
    levels = jnp.arange(FRACS, dtype=jnp.int32)
    picks = (fractions[:, None] == levels[None, :]).astype(taps_table.dtype)
    return jnp.dot(picks, taps_table, precision=HIGHEST)

def shear_rows(field_rows, offsets, tap_weights):
    padded = jnp.pad(field_rows, ((0, 0), (REACH, REACH)))
    columns = field_rows.shape[1]

    def one_plane(plane_line, offset, weights_here):
        summed = jnp.zeros((columns,), plane_line.dtype)
        for tap_index in range(TAPS):
            start_col = (REACH + offset + tap_index - 1).astype(jnp.int32)
            summed = summed + weights_here[tap_index] * lax.dynamic_slice_in_dim(plane_line, start_col, columns)
        return summed
    return jax.vmap(one_plane)(padded, offsets, tap_weights)

def unshear_rows(grad_rows, offsets, tap_weights):
    padded = jnp.pad(grad_rows, ((0, 0), (REACH, REACH)))
    columns = grad_rows.shape[1]

    def one_plane(plane_line, offset, weights_here):
        summed = jnp.zeros((columns,), plane_line.dtype)
        for tap_index in range(TAPS):
            start_col = (REACH - offset - tap_index + 1).astype(jnp.int32)
            summed = summed + weights_here[tap_index] * lax.dynamic_slice_in_dim(plane_line, start_col, columns)
        return summed
    return jax.vmap(one_plane)(padded, offsets, tap_weights)

def row_gradients(emission_row, absorption_row, goal_row, offsets, tap_weights):
    color_raw = shear_rows(emission_row, offsets, tap_weights)
    density = shear_rows(absorption_row, offsets, tap_weights)
    optical = jax.nn.softplus(density) / NZ
    transmit = jnp.exp(optical - jnp.cumsum(optical, axis=0))
    opacity = -jnp.expm1(-optical)
    emitted = transmit * opacity * color_raw
    rendered = lax.optimization_barrier(jnp.sum(emitted, axis=0))
    behind = rendered[None, :] - jnp.cumsum(emitted, axis=0)
    residual = rendered - goal_row
    grad_color = NZ * residual[None, :] * transmit * opacity
    grad_density = residual[None, :] * (transmit * jnp.exp(-optical) * color_raw - behind) * jax.nn.sigmoid(density)
    return (unshear_rows(grad_color, offsets, tap_weights), unshear_rows(grad_density, offsets, tap_weights))

def reference(emission, absorption, target, shift_whole, shift_fraction, taps_table):
    taps_all = [plane_taps(shift_fraction[view_index], taps_table) for view_index in range(ITERS)]

    def fit_row(row_index, carried):
        out_emission, out_absorption = carried
        emission_row = lax.dynamic_index_in_dim(emission, row_index, 1, keepdims=False)
        absorption_row = lax.dynamic_index_in_dim(absorption, row_index, 1, keepdims=False)
        goal_rows = lax.dynamic_index_in_dim(target, row_index, 1, keepdims=False)
        fields = [emission_row, absorption_row]
        moments_first = [jnp.zeros_like(emission_row), jnp.zeros_like(emission_row)]
        moments_second = [jnp.zeros_like(emission_row), jnp.zeros_like(emission_row)]
        for view_index in range(ITERS):
            gradients = row_gradients(fields[0], fields[1], goal_rows[view_index], shift_whole[view_index], taps_all[view_index])
            step_number = view_index + 1
            for which in range(2):
                moments_first[which] = BETA_FIRST * moments_first[which] + (1.0 - BETA_FIRST) * gradients[which]
                moments_second[which] = BETA_SECOND * moments_second[which] + (1.0 - BETA_SECOND) * gradients[which] * gradients[which]
                scaled_first = moments_first[which] / (1.0 - BETA_FIRST ** step_number)
                scaled_second = moments_second[which] / (1.0 - BETA_SECOND ** step_number)
                fields[which] = fields[which] - LEARN_RATE * scaled_first / (jnp.sqrt(scaled_second) + ADAM_EPSILON)
        out_emission = lax.dynamic_update_index_in_dim(out_emission, fields[0], row_index, 1)
        out_absorption = lax.dynamic_update_index_in_dim(out_absorption, fields[1], row_index, 1)
        return (out_emission, out_absorption)
    fitted_emission, fitted_absorption = lax.fori_loop(jnp.int32(0), jnp.int32(R), fit_row, (jnp.zeros_like(emission), jnp.zeros_like(absorption)))
    return (fitted_emission, fitted_absorption)
```

```python
import functools

import jax
import jax.numpy as jnp
from jax import lax
from jax.experimental import pallas as pl
from jax.experimental.pallas import tpu as pltpu
from jax.sharding import PartitionSpec as P

ITERS = 3
LEARN_RATE = 0.1
BETA_FIRST = 0.9
BETA_SECOND = 0.999
ADAM_EPSILON = 0.001

LANES = 128
HALF = 8
TOP = 8
PADDED = 32
GROUP = 8
INTERPRET = False


def halves(ref, *lead):
    return [ref[(*lead, pl.ds(HALF * h, HALF), slice(None))] for h in range(2)]


def put_halves(ref, lead, values):
    for h in range(2):
        ref[(*lead, pl.ds(HALF * h, HALF), slice(None))] = values[h]


def resampled(buf, lead, start, step, weights, lane):
    rows = {
        d: [buf[(*lead, pl.ds(TOP + HALF * h + d, HALF), slice(None))] for h in range(2)]
        for d in (-1, 0, 1)
    }
    total = [None, None]
    for k, weight in enumerate(weights):
        lag = start + step * k
        low = lane < lag
        high = lane >= lag + LANES
        turn = (LANES - lag) & (LANES - 1)
        for h in range(2):
            picked = jnp.where(low, rows[1][h], jnp.where(high, rows[-1][h], rows[0][h]))
            term = weight * pltpu.roll(picked, turn, 1)
            total[h] = term if total[h] is None else total[h] + term
    return total


def plane_weights(fraction_ref, table_ref, view, z):
    row = fraction_ref[view, z]
    return [table_ref[row, k] for k in range(table_ref.shape[1])]


def adam_change(view, grad, first):
    power = view + 1
    if view == 0:
        return LEARN_RATE * grad / (jnp.abs(grad) + ADAM_EPSILON)
    top = grad
    square = grad * grad
    for age, old in enumerate(first):
        top = top + BETA_FIRST ** (age + 1) * old
        square = square + BETA_SECOND ** (age + 1) * (old * old)
    top = top * (LEARN_RATE * (1.0 - BETA_FIRST) / (1.0 - BETA_FIRST**power))
    square = square * ((1.0 - BETA_SECOND) / (1.0 - BETA_SECOND**power))
    return top / (jnp.sqrt(square) + ADAM_EPSILON)


def march(color, density, carry, planes):
    depth, passing, light = carry
    fade = jnp.exp(-jnp.abs(density))
    optical = (jnp.maximum(density, 0.0) + jnp.log1p(fade)) * (1.0 / planes)
    inverse = 1.0 / (1.0 + fade)
    slope = jnp.where(density >= 0.0, inverse, fade * inverse)
    small = optical * (1.0 - optical * (0.5 - optical * (1.0 / 6.0 - optical * (1.0 / 24.0))))
    opacity = jnp.where(optical < 0.03, small, 1.0 - jnp.exp(-optical))
    blend = passing * opacity
    depth = depth + optical
    passing = jnp.exp(-depth)
    light = light + blend * color
    reach = slope * (passing * color + light)
    return (depth, passing, light), (blend, reach, slope)


def clear_edges(buf):
    blank = jnp.zeros((HALF, LANES), jnp.float32)
    for p in range(buf.shape[0]):
        for f in range(buf.shape[1]):
            buf[p, f, pl.ds(0, TOP), :] = blank
            buf[p, f, pl.ds(TOP + 2 * HALF, HALF), :] = blank


def lane_index():
    return lax.broadcasted_iota(jnp.int32, (HALF, LANES), 1)


def fresh_carry():
    zero = jnp.zeros((HALF, LANES), jnp.float32)
    return [(zero, zero + 1.0, zero) for _ in range(2)]


def forward_group(view, base, buf, carry, scalars, outs, lane, planes):
    shift_ref, fraction_ref, table_ref = scalars
    for p in range(GROUP):
        z = base + p
        weights = plane_weights(fraction_ref, table_ref, view, z)
        start = shift_ref[view, z] - 1
        color = resampled(buf, (p, 0), start, 1, weights, lane)
        density = resampled(buf, (p, 1), start, 1, weights, lane)
        for h in range(2):
            carry[h], kept = march(color[h], density[h], carry[h], planes)
            for ref, value in zip(outs, kept):
                ref[z, pl.ds(HALF * h, HALF), :] = value
    return carry


def put_slab(slab_ref, carry):
    put_halves(slab_ref, (0,), [carry[h][2] for h in range(2)])
    put_halves(slab_ref, (1,), [carry[h][0] for h in range(2)])


def first_kernel(planes, shift_ref, fraction_ref, table_ref, sent_ref, e_ref, a_ref, goal_ref,
                 blend_ref, reach_ref, slope_ref, slab_ref, buf, sems):
    depth_planes = e_ref.shape[0]
    tiles = e_ref.shape[1]
    copies = []
    for t in range(tiles):
        for f, ref in enumerate((e_ref, a_ref)):
            copies.append(pltpu.make_async_copy(
                sent_ref.at[t, pl.ds(f * depth_planes, depth_planes), :], ref.at[:, t, :], sems.at[f, t]))
        copies.append(pltpu.make_async_copy(
            sent_ref.at[t, pl.ds(2 * depth_planes, ITERS), :], goal_ref.at[:, t, :], sems.at[2, t]))
    for c in copies:
        c.start()
    clear_edges(buf)
    lane = lane_index()
    for c in copies:
        c.wait()

    def step(i, carry):
        base = i * GROUP
        for p in range(GROUP):
            for f, ref in enumerate((e_ref, a_ref)):
                for h in range(2):
                    buf[p, f, pl.ds(TOP + HALF * h, HALF), :] = ref[base + p, pl.ds(HALF * h, HALF), :]
        return forward_group(0, base, buf, list(carry), (shift_ref, fraction_ref, table_ref),
                             (blend_ref, reach_ref, slope_ref), lane, planes)

    put_slab(slab_ref, lax.fori_loop(0, depth_planes // GROUP, step, fresh_carry()))


def combined_rays(view, here_ref, slabs_ref, goal_ref, planes):
    here = here_ref[0]
    found = []
    for h in range(2):
        rows = pl.ds(HALF * h, HALF)
        depth = jnp.zeros((HALF, LANES), jnp.float32)
        image = depth
        front = depth
        clear = depth + 1.0
        passing = clear
        for i in range(slabs_ref.shape[0]):
            front = jnp.where(here == i, image, front)
            clear = jnp.where(here == i, passing, clear)
            image = image + passing * slabs_ref[i, 0, rows, :]
            depth = depth + slabs_ref[i, 1, rows, :]
            passing = jnp.exp(-depth)
        residual = image - goal_ref[view, rows, :]
        found.append((residual * clear, residual * (image - front)))
    return found


def later_kernel(view, planes, *refs):
    last = view == ITERS - 1
    here_ref, shift_ref, fraction_ref, table_ref, slabs_ref, goal_ref = refs[:6]
    at = 6
    fields = refs[at : at + 2]
    at += 2
    old = [refs[at + 2 * n : at + 2 * n + 2] for n in range(view)][::-1]
    at += 2 * view
    kept = refs[at : at + 3]
    at += 3
    new_fields = refs[at : at + 2]
    at += 2
    if last:
        sent_ref = new_fields[0]
        at -= 1
    else:
        grads = refs[at : at + 2]
        new_kept = refs[at + 2 : at + 5]
        slab_ref = refs[at + 5]
        at += 6
    if last:
        gbuf, store_e, store_a, sems = refs[at:]
        new_fields = (store_e, store_a)
    else:
        gbuf, fbuf = refs[at:]
        clear_edges(fbuf)
    clear_edges(gbuf)
    lane = lane_index()
    rays = combined_rays(view, here_ref, slabs_ref, goal_ref, planes)
    depth_planes = fields[0].shape[0]

    def step(i, carry):
        base = i * GROUP
        for p in range(GROUP):
            for h in range(2):
                rows = pl.ds(HALF * h, HALF)
                blend, reach, slope = (ref[base + p, rows, :] for ref in kept)
                near, far = rays[h]
                gbuf[p, 0, pl.ds(TOP + HALF * h, HALF), :] = (near * planes) * blend
                gbuf[p, 1, pl.ds(TOP + HALF * h, HALF), :] = near * reach - far * slope
        for p in range(GROUP):
            z = base + p
            weights = plane_weights(fraction_ref, table_ref, view, z)
            start = 1 - shift_ref[view, z]
            for f in range(2):
                grad = resampled(gbuf, (p, f), start, -1, weights, lane)
                for h in range(2):
                    rows = pl.ds(HALF * h, HALF)
                    first = [pair[f][z, rows, :] for pair in old]
                    value = fields[f][z, rows, :] - adam_change(view, grad[h], first)
                    new_fields[f][z, rows, :] = value
                    if not last:
                        grads[f][z, rows, :] = grad[h]
                        fbuf[p, f, pl.ds(TOP + HALF * h, HALF), :] = value
        if last:
            return carry
        return forward_group(view + 1, base, fbuf, list(carry), (shift_ref, fraction_ref, table_ref),
                             new_kept, lane, planes)

    if last:
        lax.fori_loop(0, depth_planes // GROUP, step, 0)
        copies = [
            pltpu.make_async_copy(
                ref.at[:, t, :], sent_ref.at[t, pl.ds(f * depth_planes, depth_planes), :], sems.at[f, t])
            for t in range(sent_ref.shape[0])
            for f, ref in enumerate(new_fields)
        ]
        for c in copies:
            c.start()
        for c in copies:
            c.wait()
    else:
        put_slab(slab_ref, lax.fori_loop(0, depth_planes // GROUP, step, fresh_carry()))


def pack_kernel(e_ref, a_ref, goal_ref, sent_ref, sems):
    depth_planes = e_ref.shape[0]
    copies = []
    for t in range(e_ref.shape[1]):
        for f, ref in enumerate((e_ref, a_ref)):
            copies.append(pltpu.make_async_copy(
                ref.at[:, t, :], sent_ref.at[t, pl.ds(f * depth_planes, depth_planes), :], sems.at[f, t]))
        copies.append(pltpu.make_async_copy(
            goal_ref.at[:, t, :], sent_ref.at[t, pl.ds(2 * depth_planes, ITERS), :], sems.at[2, t]))
    for c in copies:
        c.start()
    for c in copies:
        c.wait()


def unpack_kernel(sent_ref, e_ref, a_ref, sems):
    depth_planes = e_ref.shape[0]
    copies = [
        pltpu.make_async_copy(
            sent_ref.at[t, pl.ds(f * depth_planes, depth_planes), :], ref.at[:, t, :], sems.at[f, t])
        for t in range(e_ref.shape[1])
        for f, ref in enumerate((e_ref, a_ref))
    ]
    for c in copies:
        c.start()
    for c in copies:
        c.wait()


ANY = pl.BlockSpec(memory_space=pl.ANY)
VMEM = pl.BlockSpec(memory_space=pltpu.VMEM)
SMEM = pl.BlockSpec(memory_space=pltpu.SMEM)


def call(kernel, in_specs, out_specs, out_shape, scratch, name):
    return pl.pallas_call(
        kernel,
        in_specs=in_specs,
        out_specs=out_specs,
        out_shape=out_shape,
        scratch_shapes=scratch,
        interpret=INTERPRET,
        name=name,
        compiler_params=pltpu.CompilerParams(vmem_limit_bytes=40 * 1024 * 1024),
    )


def body(emission, absorption, target, shift_whole, shift_fraction, taps_table):
    depth_planes, tiles, width = emission.shape
    slabs = lax.axis_size("depth")
    planes = depth_planes * slabs
    here = lax.axis_index("depth").astype(jnp.int32).reshape(1)
    scalars = (shift_whole, shift_fraction, taps_table)
    volume = jax.ShapeDtypeStruct(emission.shape, jnp.float32)
    slab = jax.ShapeDtypeStruct((2, tiles, width), jnp.float32)
    goals = jax.ShapeDtypeStruct((ITERS, tiles, width), jnp.float32)
    padded = pltpu.VMEM((GROUP, 2, PADDED, width), jnp.float32)

    def sems(n):
        return pltpu.SemaphoreType.DMA((n, tiles))

    packed_rows = 2 * depth_planes + 8
    packed = call(
        pack_kernel, [ANY] * 3, ANY, jax.ShapeDtypeStruct((tiles, packed_rows, width), jnp.float32),
        [sems(3)], "pack",
    )(emission, absorption, target)
    packed = lax.all_to_all(packed, "lat", 0, 0, tiled=True)
    e, a, goal, *kept, sums = call(
        functools.partial(first_kernel, planes),
        [SMEM] * 3 + [ANY], [VMEM] * 7,
        [volume, volume, goals, volume, volume, volume, slab],
        [padded, sems(3)], "first",
    )(*scalars, packed)
    old = []
    for view in range(ITERS):
        everyone = lax.all_to_all(
            jnp.broadcast_to(sums[None], (slabs, *sums.shape)), "depth", 0, 0, tiled=True)
        last = view == ITERS - 1
        operands = (here, *scalars, everyone, goal, e, a, *old, *kept)
        in_specs = [SMEM] * 4 + [VMEM] * (len(operands) - 4)
        kernel = functools.partial(later_kernel, view, planes)
        if last:
            packed = call(
                kernel, in_specs, ANY, jax.ShapeDtypeStruct((tiles, 2 * depth_planes, width), jnp.float32),
                [padded, pltpu.VMEM(emission.shape, jnp.float32), pltpu.VMEM(emission.shape, jnp.float32), sems(2)],
                "last",
            )(*operands)
        else:
            e, a, g_e, g_a, *kept, sums = call(
                kernel, in_specs, [VMEM] * 8, [volume] * 7 + [slab], [padded, padded], "middle",
            )(*operands)
            old = [*old, g_e, g_a]
    packed = lax.all_to_all(packed, "lat", 0, 0, tiled=True)
    return call(unpack_kernel, [ANY], [ANY, ANY], [volume, volume], [sems(2)], "unpack")(packed)


def solution(mesh):
    in_specs = (
        P("depth", None, "lat"),
        P("depth", None, "lat"),
        P(None, None, "lat"),
        P(None, "depth"),
        P(None, "depth"),
        P(),
    )
    out_specs = (P("depth", None, "lat"), P("depth", None, "lat"))
    return jax.shard_map(body, mesh=mesh, in_specs=in_specs, out_specs=out_specs, check_vma=False)
```

```python
import functools

import jax
import jax.numpy as jnp
from jax import lax
from jax.experimental import pallas as pl
from jax.experimental.pallas import tpu as pltpu
from jax.sharding import PartitionSpec as P

ITERS = 3
LEARN_RATE = 0.1
BETA_FIRST = 0.9
BETA_SECOND = 0.999
ADAM_EPSILON = 0.001
LOG2E = 1.4426950408889634

LANES = 128
HALF = 8
TOP = 8
PADDED = 32
GROUP = 16
CHUNKS = 4
INTERPRET = False


def halves(ref, *lead):
    return [ref[(*lead, pl.ds(HALF * h, HALF), slice(None))] for h in range(2)]


def put_halves(ref, lead, values):
    for h in range(2):
        ref[(*lead, pl.ds(HALF * h, HALF), slice(None))] = values[h]


def resampled(buf, lead, start, step, weights, lane):
    total = [None, None]
    for k, weight in enumerate(weights):
        lag = start + step * k
        behind = lag >> 31
        wrapped = lane < (lag & (LANES - 1))
        turn = (-lag) & (LANES - 1)
        for h in range(2):
            here = buf[(*lead, pl.ds(behind + (TOP + HALF * h), HALF), slice(None))]
            after = buf[(*lead, pl.ds(behind + (TOP + HALF * h + 1), HALF), slice(None))]
            term = weight * pltpu.roll(jnp.where(wrapped, after, here), turn, 1)
            total[h] = term if total[h] is None else total[h] + term
    return total


def plane_weights(fraction_ref, table_ref, view, z):
    column = fraction_ref[view, z]
    return [table_ref[k, column] for k in range(table_ref.shape[0])]


def adam_change(view, grad, first):
    power = view + 1
    if view == 0:
        return LEARN_RATE * grad / (jnp.abs(grad) + ADAM_EPSILON)
    top = grad
    square = grad * grad
    for age, old in enumerate(first):
        top = top + BETA_FIRST ** (age + 1) * old
        square = square + BETA_SECOND ** (age + 1) * (old * old)
    top = top * (LEARN_RATE * (1.0 - BETA_FIRST) / (1.0 - BETA_FIRST**power))
    square = square * ((1.0 - BETA_SECOND) / (1.0 - BETA_SECOND**power))
    return top / (jnp.sqrt(square) + ADAM_EPSILON)


def march(color, density, carry, planes):
    depth, passing, light = carry
    density = density * LOG2E
    fade = jnp.exp2(-jnp.abs(density))
    whole = 1.0 + fade
    soft = jnp.maximum(density, 0.0) + (jnp.log2(whole) + (fade - (whole - 1.0)) * LOG2E)
    slope = jnp.exp2(density - soft)
    optical = soft * (1.0 / (planes * LOG2E))
    series = optical * (1.0 - optical * (0.5 - optical * (1.0 / 6.0)))
    opacity = jnp.where(optical < 0.01, series, 1.0 - jnp.exp2(soft * (-1.0 / planes)))
    blend = passing * opacity
    depth = depth + soft
    passing = jnp.exp2(depth * (-1.0 / planes))
    light = light + blend * color
    reach = slope * (passing * color + light)
    return (depth, passing, light), (blend, reach, slope)


def clear_edges(buf):
    blank = jnp.zeros((HALF, LANES), jnp.float32)
    for p in range(buf.shape[0]):
        for f in range(buf.shape[1]):
            buf[p, f, pl.ds(0, TOP), :] = blank
            buf[p, f, pl.ds(TOP + 2 * HALF, HALF), :] = blank


def lane_index():
    return lax.broadcasted_iota(jnp.int32, (HALF, LANES), 1)


def fresh_carry():
    zero = jnp.zeros((HALF, LANES), jnp.float32)
    return [(zero, zero + 1.0, zero) for _ in range(2)]


def forward_group(view, base, buf, carry, scalars, outs, lane, planes):
    shift_ref, fraction_ref, table_ref = scalars
    for p in range(GROUP):
        z = base + p
        weights = plane_weights(fraction_ref, table_ref, view, z)
        start = shift_ref[view, z] - 1
        color = resampled(buf, (p, 0), start, 1, weights, lane)
        density = resampled(buf, (p, 1), start, 1, weights, lane)
        for h in range(2):
            carry[h], kept = march(color[h], density[h], carry[h], planes)
            for ref, value in zip(outs, kept):
                ref[z, pl.ds(HALF * h, HALF), :] = value
    return carry


def put_slab(slab_ref, carry):
    for i in range(slab_ref.shape[0]):
        put_halves(slab_ref, (i, 0), [carry[h][2] for h in range(2)])
        put_halves(slab_ref, (i, 1), [carry[h][0] for h in range(2)])


def first_kernel(planes, shift_ref, fraction_ref, table_ref, sent_ref, e_ref, a_ref, goal_ref,
                 blend_ref, reach_ref, slope_ref, slab_ref, buf):
    depth_planes = e_ref.shape[0]
    clear_edges(buf)
    lane = lane_index()
    for t in range(goal_ref.shape[1]):
        goal_ref[:, t, :] = sent_ref[t, pl.ds(2 * depth_planes, ITERS), :]

    def step(i, carry):
        base = pl.multiple_of(i * GROUP, GROUP)
        for f, ref in enumerate((e_ref, a_ref)):
            for g in range(GROUP // HALF):
                for h in range(2):
                    rows = pl.ds(HALF * h, HALF)
                    block = jnp.transpose(
                        sent_ref[rows, pl.ds(f * depth_planes + base + g * HALF, HALF), :], (1, 0, 2))
                    ref[pl.ds(base + g * HALF, HALF), rows, :] = block
                    buf[pl.ds(g * HALF, HALF), f, pl.ds(TOP + HALF * h, HALF), :] = block
        return forward_group(0, base, buf, list(carry), (shift_ref, fraction_ref, table_ref),
                             (blend_ref, reach_ref, slope_ref), lane, planes)

    put_slab(slab_ref, lax.fori_loop(0, depth_planes // GROUP, step, fresh_carry()))


def combined_rays(view, slabs_ref, goal_ref, planes):
    here = lax.axis_index("depth")
    found = []
    for h in range(2):
        rows = pl.ds(HALF * h, HALF)
        depth = jnp.zeros((HALF, LANES), jnp.float32)
        image = depth
        front = depth
        clear = depth + 1.0
        passing = clear
        for i in range(slabs_ref.shape[0]):
            front = jnp.where(here == i, image, front)
            clear = jnp.where(here == i, passing, clear)
            image = image + passing * slabs_ref[i, 0, rows, :]
            depth = depth + slabs_ref[i, 1, rows, :]
            passing = jnp.exp2(depth * (-1.0 / planes))
        residual = image - goal_ref[view, rows, :]
        near = residual * clear
        found.append((near * planes, near, residual * (image - front)))
    return found


def later_kernel(view, planes, *refs):
    last = view == ITERS - 1
    refs = list(refs)

    def take(n):
        taken = refs[:n]
        del refs[:n]
        return taken

    shift_ref, fraction_ref, table_ref, slabs_ref, goal_ref = take(5)
    fields = take(2)
    old = [take(2) for _ in range(view)][::-1]
    kept = take(3)
    if last:
        (sent_ref,) = take(1)
        gbuf, fbuf = refs
    else:
        new_fields, grads, new_kept, (slab_ref,) = take(2), take(2), take(3), take(1)
        gbuf, fbuf = refs
        clear_edges(fbuf)
    clear_edges(gbuf)
    lane = lane_index()
    rays = combined_rays(view, slabs_ref, goal_ref, planes)
    depth_planes = fields[0].shape[0]

    def step(i, carry):
        base = pl.multiple_of(i * GROUP, GROUP)
        for p in range(GROUP):
            for h in range(2):
                rows = pl.ds(HALF * h, HALF)
                blend, reach, slope = (ref[base + p, rows, :] for ref in kept)
                scaled, near, far = rays[h]
                gbuf[p, 0, pl.ds(TOP + HALF * h, HALF), :] = scaled * blend
                gbuf[p, 1, pl.ds(TOP + HALF * h, HALF), :] = near * reach - far * slope
        for p in range(GROUP):
            z = base + p
            weights = plane_weights(fraction_ref, table_ref, view, z)
            start = 1 - shift_ref[view, z]
            for f in range(2):
                grad = resampled(gbuf, (p, f), start, -1, weights, lane)
                for h in range(2):
                    rows = pl.ds(HALF * h, HALF)
                    first = [pair[f][z, rows, :] for pair in old]
                    value = fields[f][z, rows, :] - adam_change(view, grad[h], first)
                    fbuf[p, f, pl.ds(TOP + HALF * h, HALF), :] = value
                    if not last:
                        new_fields[f][z, rows, :] = value
                        grads[f][z, rows, :] = grad[h]
        if last:
            for f in range(2):
                for g in range(GROUP // HALF):
                    for h in range(2):
                        block = fbuf[pl.ds(g * HALF, HALF), f, pl.ds(TOP + HALF * h, HALF), :]
                        sent_ref[pl.ds(HALF * h, HALF), pl.ds(f * depth_planes + base + g * HALF, HALF), :] = (
                            jnp.transpose(block, (1, 0, 2)))
            return carry
        return forward_group(view + 1, base, fbuf, list(carry), (shift_ref, fraction_ref, table_ref),
                             new_kept, lane, planes)

    if last:
        lax.fori_loop(0, depth_planes // GROUP, step, 0)
    else:
        put_slab(slab_ref, lax.fori_loop(0, depth_planes // GROUP, step, fresh_carry()))


def pack_kernel(e_ref, a_ref, goal_ref, shift_ref, fraction_ref, table_ref,
                sent_ref, shift_out, fraction_out, table_out,
                e_buf, a_buf, goal_buf, sems, small_sems):
    depth_planes = e_ref.shape[0]
    span = depth_planes // CHUNKS
    copies = [
        [pltpu.make_async_copy(ref.at[pl.ds(c * span, span)], buf.at[pl.ds(c * span, span)], sems.at[f, c])
         for c in range(CHUNKS)]
        for f, (ref, buf) in enumerate(((e_ref, e_buf), (a_ref, a_buf)))
    ]
    small = [
        pltpu.make_async_copy(ref, buf, small_sems.at[n])
        for n, (ref, buf) in enumerate((
            (goal_ref, goal_buf), (shift_ref, shift_out), (fraction_ref, fraction_out), (table_ref, table_out)))
    ]
    for c in [*copies[0], *copies[1], *small]:
        c.start()
    for f, buf in enumerate((e_buf, a_buf)):
        for c in range(CHUNKS):
            copies[f][c].wait()
            for g in range(span // HALF):
                z = c * span + g * HALF
                for h in range(2):
                    rows = pl.ds(HALF * h, HALF)
                    sent_ref[rows, pl.ds(f * depth_planes + z, HALF), :] = jnp.transpose(
                        buf[pl.ds(z, HALF), rows, :], (1, 0, 2))
    for c in small:
        c.wait()
    for t in range(goal_ref.shape[1]):
        sent_ref[t, pl.ds(2 * depth_planes, ITERS), :] = goal_buf[:, t, :]


def unpack_kernel(sent_ref, e_ref, a_ref, e_buf, a_buf, sems):
    depth_planes = e_ref.shape[0]
    span = depth_planes // CHUNKS
    copies = []
    for f, (ref, buf) in enumerate(((e_ref, e_buf), (a_ref, a_buf))):
        for c in range(CHUNKS):
            for g in range(span // HALF):
                z = c * span + g * HALF
                for h in range(2):
                    rows = pl.ds(HALF * h, HALF)
                    buf[pl.ds(z, HALF), rows, :] = jnp.transpose(
                        sent_ref[rows, pl.ds(f * depth_planes + z, HALF), :], (1, 0, 2))
            copy = pltpu.make_async_copy(
                buf.at[pl.ds(c * span, span)], ref.at[pl.ds(c * span, span)], sems.at[f, c])
            copy.start()
            copies.append(copy)
    for copy in copies:
        copy.wait()


HBM = pl.BlockSpec(memory_space=pltpu.HBM)
VMEM = pl.BlockSpec(memory_space=pltpu.VMEM)
SMEM = pl.BlockSpec(memory_space=pltpu.SMEM)


def call(kernel, in_specs, out_specs, out_shape, scratch, name):
    return pl.pallas_call(
        kernel,
        in_specs=in_specs,
        out_specs=out_specs,
        out_shape=out_shape,
        scratch_shapes=scratch,
        interpret=INTERPRET,
        name=name,
        compiler_params=pltpu.CompilerParams(vmem_limit_bytes=16 * 1024 * 1024),
    )


def body(emission, absorption, target, shift_whole, shift_fraction, taps_table):
    depth_planes, tiles, width = emission.shape
    slabs = lax.axis_size("depth")
    planes = depth_planes * slabs
    volume = jax.ShapeDtypeStruct(emission.shape, jnp.float32)
    slab = jax.ShapeDtypeStruct((slabs, 2, tiles, width), jnp.float32)
    goals = jax.ShapeDtypeStruct((ITERS, tiles, width), jnp.float32)
    padded = pltpu.VMEM((GROUP, 2, PADDED, width), jnp.float32)
    store = pltpu.VMEM(emission.shape, jnp.float32)
    sems = pltpu.SemaphoreType.DMA((2, CHUNKS))

    raw = [
        pltpu.with_memory_space_constraint(x, pltpu.HBM)
        for x in (emission, absorption, target, shift_whole, shift_fraction, taps_table.T)
    ]
    packed, *scalars = call(
        pack_kernel, [HBM] * 6, [VMEM] * 4,
        [jax.ShapeDtypeStruct((tiles, 2 * depth_planes + HALF, width), jnp.float32)]
        + [jax.ShapeDtypeStruct(x.shape, x.dtype) for x in raw[3:]],
        [store, store, pltpu.VMEM(target.shape, jnp.float32), sems, pltpu.SemaphoreType.DMA((4,))], "pack",
    )(*raw)
    packed = lax.all_to_all(packed, "lat", 0, 0, tiled=True)
    e, a, goal, *kept, sums = call(
        functools.partial(first_kernel, planes), [SMEM] * 3 + [VMEM], [VMEM] * 7,
        [volume, volume, goals, volume, volume, volume, slab], [padded], "first",
    )(*scalars, packed)
    old = []
    for view in range(ITERS):
        everyone = lax.all_to_all(sums, "depth", 0, 0, tiled=True)
        operands = (*scalars, everyone, goal, e, a, *old, *kept)
        in_specs = [SMEM] * 3 + [VMEM] * (len(operands) - 3)
        kernel = functools.partial(later_kernel, view, planes)
        if view == ITERS - 1:
            packed = call(
                kernel, in_specs, VMEM,
                jax.ShapeDtypeStruct((tiles, 2 * depth_planes, width), jnp.float32), [padded, padded], "last",
            )(*operands)
        else:
            e, a, g_e, g_a, *kept, sums = call(
                kernel, in_specs, [VMEM] * 8, [volume] * 7 + [slab], [padded, padded], "middle",
            )(*operands)
            old = [*old, g_e, g_a]
    packed = lax.all_to_all(packed, "lat", 0, 0, tiled=True)
    return call(
        unpack_kernel, [VMEM], [HBM, HBM], [volume, volume], [store, store, sems], "unpack")(packed)


def solution(mesh):
    in_specs = (
        P("depth", None, "lat"),
        P("depth", None, "lat"),
        P(None, None, "lat"),
        P(None, "depth"),
        P(None, "depth"),
        P(),
    )
    out_specs = (P("depth", None, "lat"), P("depth", None, "lat"))
    return jax.shard_map(body, mesh=mesh, in_specs=in_specs, out_specs=out_specs, check_vma=False)
```

```python
import functools
import math

import jax
import jax.numpy as jnp
from jax import lax
from jax.experimental import pallas as pl
from jax.experimental.pallas import tpu as pltpu
from jax.sharding import PartitionSpec as P

ITERS = 3
LEARN_RATE = 0.1
BETA_FIRST = 0.9
BETA_SECOND = 0.999
ADAM_EPSILON = 0.001
LOG2E = 1.4426950408889634
TINY = 1e-37

LANES = 128
HALF = 8
TOP = 8
PADDED = 32
GROUP = 32
CHUNKS = 4
INTERPRET = False


def halves(ref, *lead):
    return [ref[(*lead, pl.ds(HALF * h, HALF), slice(None))] for h in range(2)]


def put_halves(ref, lead, values):
    for h in range(2):
        ref[(*lead, pl.ds(HALF * h, HALF), slice(None))] = values[h]


def resampled(buf, lead, start, step, weights, lane):
    total = [None, None]
    for k, weight in enumerate(weights):
        lag = start + step * k
        behind = lag >> 31
        wrapped = lane < (lag & (LANES - 1))
        turn = (-lag) & (LANES - 1)
        for h in range(2):
            here = buf[(*lead, pl.ds(behind + (TOP + HALF * h), HALF), slice(None))]
            after = buf[(*lead, pl.ds(behind + (TOP + HALF * h + 1), HALF), slice(None))]
            term = weight * pltpu.roll(jnp.where(wrapped, after, here), turn, 1)
            total[h] = term if total[h] is None else total[h] + term
    return total


def plane_weights(fraction_ref, table_ref, view, z):
    column = fraction_ref[view, z]
    return [table_ref[k, column] for k in range(table_ref.shape[0])]


def adam_change(view, grad, first):
    power = view + 1
    if view == 0:
        return LEARN_RATE * grad / (jnp.abs(grad) + ADAM_EPSILON)
    top = grad
    square = grad * grad
    for age, old in enumerate(first):
        top = top + BETA_FIRST ** (age + 1) * old
        square = square + BETA_SECOND ** (age + 1) * (old * old)
    scale = math.sqrt((1.0 - BETA_SECOND) / (1.0 - BETA_SECOND**power))
    rate = LEARN_RATE * (1.0 - BETA_FIRST) / (1.0 - BETA_FIRST**power) / scale
    root = square * lax.rsqrt(jnp.maximum(square, TINY))
    return rate * top / (root + ADAM_EPSILON / scale)


def march(color, density, carry, planes):
    passing, light = carry
    density = density * LOG2E
    fade = jnp.exp2(-jnp.abs(density))
    soft = jnp.maximum(density, 0.0) + jnp.log2(1.0 + fade)
    slope = jnp.exp2(density - soft)
    unit = 1.0 / (planes * LOG2E)
    opacity = soft * (unit - soft * (unit**2 / 2.0 - soft * (unit**3 / 6.0)))
    blend = passing * opacity
    passing = passing - blend
    light = light + blend * color
    reach = slope * (passing * color + light)
    return (passing, light), (blend, reach, slope)


def clear_edges(buf):
    blank = jnp.zeros((HALF, LANES), jnp.float32)
    for p in range(buf.shape[0]):
        for f in range(buf.shape[1]):
            buf[p, f, pl.ds(0, TOP), :] = blank
            buf[p, f, pl.ds(TOP + 2 * HALF, HALF), :] = blank


def lane_index():
    return lax.broadcasted_iota(jnp.int32, (HALF, LANES), 1)


def fresh_carry():
    zero = jnp.zeros((HALF, LANES), jnp.float32)
    return [(zero + 1.0, zero) for _ in range(2)]


def forward_group(view, base, buf, carry, scalars, outs, lane, planes):
    shift_ref, fraction_ref, table_ref = scalars
    for p in range(GROUP):
        z = base + p
        weights = plane_weights(fraction_ref, table_ref, view, z)
        start = shift_ref[view, z] - 1
        color = resampled(buf, (p, 0), start, 1, weights, lane)
        density = resampled(buf, (p, 1), start, 1, weights, lane)
        for h in range(2):
            carry[h], kept = march(color[h], density[h], carry[h], planes)
            for ref, value in zip(outs, kept):
                ref[z, pl.ds(HALF * h, HALF), :] = value
    return carry


def put_slab(slab_ref, carry):
    for i in range(slab_ref.shape[0]):
        put_halves(slab_ref, (i, 0), [carry[h][1] for h in range(2)])
        put_halves(slab_ref, (i, 1), [carry[h][0] for h in range(2)])


def first_kernel(planes, shift_ref, fraction_ref, table_ref, sent_ref, e_ref, a_ref, goal_ref,
                 blend_ref, reach_ref, slope_ref, slab_ref, buf):
    depth_planes = e_ref.shape[0]
    clear_edges(buf)
    lane = lane_index()
    for t in range(goal_ref.shape[1]):
        goal_ref[:, t, :] = sent_ref[t, pl.ds(2 * depth_planes, ITERS), :]

    def step(i, carry):
        base = pl.multiple_of(i * GROUP, GROUP)
        for f, ref in enumerate((e_ref, a_ref)):
            for g in range(GROUP // HALF):
                for h in range(2):
                    rows = pl.ds(HALF * h, HALF)
                    block = jnp.transpose(
                        sent_ref[rows, pl.ds(f * depth_planes + base + g * HALF, HALF), :], (1, 0, 2))
                    ref[pl.ds(base + g * HALF, HALF), rows, :] = block
                    buf[pl.ds(g * HALF, HALF), f, pl.ds(TOP + HALF * h, HALF), :] = block
        return forward_group(0, base, buf, list(carry), (shift_ref, fraction_ref, table_ref),
                             (blend_ref, reach_ref, slope_ref), lane, planes)

    put_slab(slab_ref, lax.fori_loop(0, depth_planes // GROUP, step, fresh_carry()))


def combined_rays(view, slabs_ref, goal_ref, planes):
    here = lax.axis_index("depth")
    found = []
    for h in range(2):
        rows = pl.ds(HALF * h, HALF)
        image = jnp.zeros((HALF, LANES), jnp.float32)
        front = image
        passing = image + 1.0
        clear = passing
        for i in range(slabs_ref.shape[0]):
            front = jnp.where(here == i, image, front)
            clear = jnp.where(here == i, passing, clear)
            image = image + passing * slabs_ref[i, 0, rows, :]
            passing = passing * slabs_ref[i, 1, rows, :]
        residual = image - goal_ref[view, rows, :]
        near = residual * clear
        found.append((near * planes, near, residual * (image - front)))
    return found


def later_kernel(view, planes, *refs):
    last = view == ITERS - 1
    refs = list(refs)

    def take(n):
        taken = refs[:n]
        del refs[:n]
        return taken

    shift_ref, fraction_ref, table_ref, slabs_ref, goal_ref = take(5)
    fields = take(2)
    old = [take(2) for _ in range(view)][::-1]
    kept = take(3)
    if last:
        (sent_ref,) = take(1)
        gbuf, fbuf = refs
    else:
        new_fields, grads, new_kept, (slab_ref,) = take(2), take(2), take(3), take(1)
        gbuf, fbuf = refs
        clear_edges(fbuf)
    clear_edges(gbuf)
    lane = lane_index()
    rays = combined_rays(view, slabs_ref, goal_ref, planes)
    depth_planes = fields[0].shape[0]

    def step(i, carry):
        base = pl.multiple_of(i * GROUP, GROUP)
        for p in range(GROUP):
            for h in range(2):
                rows = pl.ds(HALF * h, HALF)
                blend, reach, slope = (ref[base + p, rows, :] for ref in kept)
                scaled, near, far = rays[h]
                gbuf[p, 0, pl.ds(TOP + HALF * h, HALF), :] = scaled * blend
                gbuf[p, 1, pl.ds(TOP + HALF * h, HALF), :] = near * reach - far * slope
        for p in range(GROUP):
            z = base + p
            weights = plane_weights(fraction_ref, table_ref, view, z)
            start = 1 - shift_ref[view, z]
            for f in range(2):
                grad = resampled(gbuf, (p, f), start, -1, weights, lane)
                for h in range(2):
                    rows = pl.ds(HALF * h, HALF)
                    first = [pair[f][z, rows, :] for pair in old]
                    value = fields[f][z, rows, :] - adam_change(view, grad[h], first)
                    fbuf[p, f, pl.ds(TOP + HALF * h, HALF), :] = value
                    if not last:
                        new_fields[f][z, rows, :] = value
                        grads[f][z, rows, :] = grad[h]
        if last:
            for f in range(2):
                for g in range(GROUP // HALF):
                    for h in range(2):
                        block = fbuf[pl.ds(g * HALF, HALF), f, pl.ds(TOP + HALF * h, HALF), :]
                        sent_ref[pl.ds(HALF * h, HALF), pl.ds(f * depth_planes + base + g * HALF, HALF), :] = (
                            jnp.transpose(block, (1, 0, 2)))
            return carry
        return forward_group(view + 1, base, fbuf, list(carry), (shift_ref, fraction_ref, table_ref),
                             new_kept, lane, planes)

    if last:
        lax.fori_loop(0, depth_planes // GROUP, step, 0)
    else:
        put_slab(slab_ref, lax.fori_loop(0, depth_planes // GROUP, step, fresh_carry()))


def pack_kernel(e_ref, a_ref, goal_ref, shift_ref, fraction_ref, table_ref,
                sent_ref, shift_out, fraction_out, table_out,
                e_buf, a_buf, goal_buf, sems, small_sems):
    depth_planes = e_ref.shape[0]
    span = depth_planes // CHUNKS
    copies = [
        [pltpu.make_async_copy(ref.at[pl.ds(c * span, span)], buf.at[pl.ds(c * span, span)], sems.at[f, c])
         for c in range(CHUNKS)]
        for f, (ref, buf) in enumerate(((e_ref, e_buf), (a_ref, a_buf)))
    ]
    small = [
        pltpu.make_async_copy(ref, buf, small_sems.at[n])
        for n, (ref, buf) in enumerate((
            (goal_ref, goal_buf), (shift_ref, shift_out), (fraction_ref, fraction_out), (table_ref, table_out)))
    ]
    for c in [*copies[0], *copies[1], *small]:
        c.start()
    for f, buf in enumerate((e_buf, a_buf)):
        for c in range(CHUNKS):
            copies[f][c].wait()
            for g in range(span // HALF):
                z = c * span + g * HALF
                for h in range(2):
                    rows = pl.ds(HALF * h, HALF)
                    sent_ref[rows, pl.ds(f * depth_planes + z, HALF), :] = jnp.transpose(
                        buf[pl.ds(z, HALF), rows, :], (1, 0, 2))
    for c in small:
        c.wait()
    for t in range(goal_ref.shape[1]):
        sent_ref[t, pl.ds(2 * depth_planes, ITERS), :] = goal_buf[:, t, :]


def unpack_kernel(sent_ref, e_ref, a_ref, e_buf, a_buf, sems):
    depth_planes = e_ref.shape[0]
    span = depth_planes // CHUNKS
    copies = []
    for f, (ref, buf) in enumerate(((e_ref, e_buf), (a_ref, a_buf))):
        for c in range(CHUNKS):
            for g in range(span // HALF):
                z = c * span + g * HALF
                for h in range(2):
                    rows = pl.ds(HALF * h, HALF)
                    buf[pl.ds(z, HALF), rows, :] = jnp.transpose(
                        sent_ref[rows, pl.ds(f * depth_planes + z, HALF), :], (1, 0, 2))
            copy = pltpu.make_async_copy(
                buf.at[pl.ds(c * span, span)], ref.at[pl.ds(c * span, span)], sems.at[f, c])
            copy.start()
            copies.append(copy)
    for copy in copies:
        copy.wait()


HBM = pl.BlockSpec(memory_space=pltpu.HBM)
VMEM = pl.BlockSpec(memory_space=pltpu.VMEM)
SMEM = pl.BlockSpec(memory_space=pltpu.SMEM)


def call(kernel, in_specs, out_specs, out_shape, scratch, name):
    return pl.pallas_call(
        kernel,
        in_specs=in_specs,
        out_specs=out_specs,
        out_shape=out_shape,
        scratch_shapes=scratch,
        interpret=INTERPRET,
        name=name,
        compiler_params=pltpu.CompilerParams(vmem_limit_bytes=16 * 1024 * 1024),
    )


def body(emission, absorption, target, shift_whole, shift_fraction, taps_table):
    depth_planes, tiles, width = emission.shape
    slabs = lax.axis_size("depth")
    planes = depth_planes * slabs
    volume = jax.ShapeDtypeStruct(emission.shape, jnp.float32)
    slab = jax.ShapeDtypeStruct((slabs, 2, tiles, width), jnp.float32)
    goals = jax.ShapeDtypeStruct((ITERS, tiles, width), jnp.float32)
    padded = pltpu.VMEM((GROUP, 2, PADDED, width), jnp.float32)
    store = pltpu.VMEM(emission.shape, jnp.float32)
    sems = pltpu.SemaphoreType.DMA((2, CHUNKS))

    raw = [
        pltpu.with_memory_space_constraint(x, pltpu.HBM)
        for x in (emission, absorption, target, shift_whole, shift_fraction, taps_table.T)
    ]
    packed, *scalars = call(
        pack_kernel, [HBM] * 6, [VMEM] * 4,
        [jax.ShapeDtypeStruct((tiles, 2 * depth_planes + HALF, width), jnp.float32)]
        + [jax.ShapeDtypeStruct(x.shape, x.dtype) for x in raw[3:]],
        [store, store, pltpu.VMEM(target.shape, jnp.float32), sems, pltpu.SemaphoreType.DMA((4,))], "pack",
    )(*raw)
    packed = lax.all_to_all(packed, "lat", 0, 0, tiled=True)
    e, a, goal, *kept, sums = call(
        functools.partial(first_kernel, planes), [SMEM] * 3 + [VMEM], [VMEM] * 7,
        [volume, volume, goals, volume, volume, volume, slab], [padded], "first",
    )(*scalars, packed)
    old = []
    for view in range(ITERS):
        everyone = lax.all_to_all(sums, "depth", 0, 0, tiled=True)
        operands = (*scalars, everyone, goal, e, a, *old, *kept)
        in_specs = [SMEM] * 3 + [VMEM] * (len(operands) - 3)
        kernel = functools.partial(later_kernel, view, planes)
        if view == ITERS - 1:
            packed = call(
                kernel, in_specs, VMEM,
                jax.ShapeDtypeStruct((tiles, 2 * depth_planes, width), jnp.float32), [padded, padded], "last",
            )(*operands)
        else:
            e, a, g_e, g_a, *kept, sums = call(
                kernel, in_specs, [VMEM] * 8, [volume] * 7 + [slab], [padded, padded], "middle",
            )(*operands)
            old = [*old, g_e, g_a]
    packed = lax.all_to_all(packed, "lat", 0, 0, tiled=True)
    return call(
        unpack_kernel, [VMEM], [HBM, HBM], [volume, volume], [store, store, sems], "unpack")(packed)


def solution(mesh):
    in_specs = (
        P("depth", None, "lat"),
        P("depth", None, "lat"),
        P(None, None, "lat"),
        P(None, "depth"),
        P(None, "depth"),
        P(),
    )
    out_specs = (P("depth", None, "lat"), P("depth", None, "lat"))
    return jax.shard_map(body, mesh=mesh, in_specs=in_specs, out_specs=out_specs, check_vma=False)
```

```python
import functools
import math

import jax
import jax.numpy as jnp
from jax import lax
from jax.experimental import pallas as pl
from jax.experimental.pallas import tpu as pltpu
from jax.sharding import PartitionSpec as P

ITERS = 3
LEARN_RATE = 0.1
BETA_FIRST = 0.9
BETA_SECOND = 0.999
ADAM_EPSILON = 0.001
LOG2E = 1.4426950408889634
TINY = 1e-37

LANES = 128
HALF = 8
TOP = 8
PADDED = 32
GROUP = 64
CHUNKS = 4
INTERPRET = False


def halves(ref, *lead):
    return [ref[(*lead, pl.ds(HALF * h, HALF), slice(None))] for h in range(2)]


def put_halves(ref, lead, values):
    for h in range(2):
        ref[(*lead, pl.ds(HALF * h, HALF), slice(None))] = values[h]


def resampled(buf, lead, start, step, weights, lane):
    total = [None, None]
    for k, weight in enumerate(weights):
        lag = start + step * k
        behind = lag >> 31
        wrapped = lane < (lag & (LANES - 1))
        turn = (-lag) & (LANES - 1)
        for h in range(2):
            here = buf[(*lead, pl.ds(behind + (TOP + HALF * h), HALF), slice(None))]
            after = buf[(*lead, pl.ds(behind + (TOP + HALF * h + 1), HALF), slice(None))]
            term = weight * pltpu.roll(jnp.where(wrapped, after, here), turn, 1)
            total[h] = term if total[h] is None else total[h] + term
    return total


def plane_weights(fraction_ref, table_ref, view, z):
    column = fraction_ref[view, z]
    return [table_ref[k, column] for k in range(table_ref.shape[0])]


def adam_change(view, grad, first):
    power = view + 1
    if view == 0:
        return LEARN_RATE * grad / (jnp.abs(grad) + ADAM_EPSILON)
    top = grad
    square = grad * grad
    for age, old in enumerate(first):
        top = top + BETA_FIRST ** (age + 1) * old
        square = square + BETA_SECOND ** (age + 1) * (old * old)
    scale = math.sqrt((1.0 - BETA_SECOND) / (1.0 - BETA_SECOND**power))
    rate = LEARN_RATE * (1.0 - BETA_FIRST) / (1.0 - BETA_FIRST**power) / scale
    root = square * lax.rsqrt(jnp.maximum(square, TINY))
    return rate * top / (root + ADAM_EPSILON / scale)


def march(color, density, carry, planes):
    passing, light = carry
    density = density * LOG2E
    fade = jnp.exp2(-jnp.abs(density))
    soft = jnp.maximum(density, 0.0) + jnp.log2(1.0 + fade)
    slope = jnp.exp2(density - soft)
    unit = 1.0 / (planes * LOG2E)
    opacity = soft * (unit - soft * (unit**2 / 2.0 - soft * (unit**3 / 6.0)))
    blend = passing * opacity
    passing = passing - blend
    light = light + blend * color
    reach = slope * (passing * color + light)
    return (passing, light), (blend, reach, slope)


def clear_edges(buf):
    blank = jnp.zeros((HALF, LANES), jnp.float32)
    for p in range(buf.shape[0]):
        for f in range(buf.shape[1]):
            buf[p, f, pl.ds(0, TOP), :] = blank
            buf[p, f, pl.ds(TOP + 2 * HALF, HALF), :] = blank


def lane_index():
    return lax.broadcasted_iota(jnp.int32, (HALF, LANES), 1)


def fresh_carry():
    zero = jnp.zeros((HALF, LANES), jnp.float32)
    return [(zero + 1.0, zero) for _ in range(2)]


def forward_group(view, base, buf, carry, scalars, outs, lane, planes):
    shift_ref, fraction_ref, table_ref = scalars
    for p in range(GROUP):
        z = base + p
        weights = plane_weights(fraction_ref, table_ref, view, z)
        start = shift_ref[view, z] - 1
        color = resampled(buf, (p, 0), start, 1, weights, lane)
        density = resampled(buf, (p, 1), start, 1, weights, lane)
        for h in range(2):
            carry[h], kept = march(color[h], density[h], carry[h], planes)
            for ref, value in zip(outs, kept):
                ref[z, pl.ds(HALF * h, HALF), :] = value
    return carry


def put_slab(slab_ref, carry):
    for i in range(slab_ref.shape[0]):
        put_halves(slab_ref, (i, 0), [carry[h][1] for h in range(2)])
        put_halves(slab_ref, (i, 1), [carry[h][0] for h in range(2)])


def first_kernel(planes, shift_ref, fraction_ref, table_ref, sent_ref, e_ref, a_ref, goal_ref,
                 blend_ref, reach_ref, slope_ref, slab_ref, buf):
    depth_planes = e_ref.shape[0]
    clear_edges(buf)
    lane = lane_index()
    for t in range(goal_ref.shape[1]):
        goal_ref[:, t, :] = sent_ref[t, pl.ds(2 * depth_planes, ITERS), :]

    def step(i, carry):
        base = pl.multiple_of(i * GROUP, GROUP)
        for f, ref in enumerate((e_ref, a_ref)):
            for g in range(GROUP // HALF):
                for h in range(2):
                    rows = pl.ds(HALF * h, HALF)
                    block = jnp.transpose(
                        sent_ref[rows, pl.ds(f * depth_planes + base + g * HALF, HALF), :], (1, 0, 2))
                    ref[pl.ds(base + g * HALF, HALF), rows, :] = block
                    buf[pl.ds(g * HALF, HALF), f, pl.ds(TOP + HALF * h, HALF), :] = block
        return forward_group(0, base, buf, list(carry), (shift_ref, fraction_ref, table_ref),
                             (blend_ref, reach_ref, slope_ref), lane, planes)

    put_slab(slab_ref, lax.fori_loop(0, depth_planes // GROUP, step, fresh_carry()))


def combined_rays(view, slabs_ref, goal_ref, planes):
    here = lax.axis_index("depth")
    found = []
    for h in range(2):
        rows = pl.ds(HALF * h, HALF)
        image = jnp.zeros((HALF, LANES), jnp.float32)
        front = image
        passing = image + 1.0
        clear = passing
        for i in range(slabs_ref.shape[0]):
            front = jnp.where(here == i, image, front)
            clear = jnp.where(here == i, passing, clear)
            image = image + passing * slabs_ref[i, 0, rows, :]
            passing = passing * slabs_ref[i, 1, rows, :]
        residual = image - goal_ref[view, rows, :]
        near = residual * clear
        found.append((near * planes, near, residual * (image - front)))
    return found


def later_kernel(view, planes, *refs):
    last = view == ITERS - 1
    refs = list(refs)

    def take(n):
        taken = refs[:n]
        del refs[:n]
        return taken

    shift_ref, fraction_ref, table_ref, slabs_ref, goal_ref = take(5)
    fields = take(2)
    old = [take(2) for _ in range(view)][::-1]
    kept = take(3)
    if last:
        (sent_ref,) = take(1)
        gbuf, fbuf = refs
    else:
        new_fields, grads, new_kept, (slab_ref,) = take(2), take(2), take(3), take(1)
        gbuf, fbuf = refs
        clear_edges(fbuf)
    clear_edges(gbuf)
    lane = lane_index()
    rays = combined_rays(view, slabs_ref, goal_ref, planes)
    depth_planes = fields[0].shape[0]

    def step(i, carry):
        base = pl.multiple_of(i * GROUP, GROUP)
        for p in range(GROUP):
            for h in range(2):
                rows = pl.ds(HALF * h, HALF)
                blend, reach, slope = (ref[base + p, rows, :] for ref in kept)
                scaled, near, far = rays[h]
                gbuf[p, 0, pl.ds(TOP + HALF * h, HALF), :] = scaled * blend
                gbuf[p, 1, pl.ds(TOP + HALF * h, HALF), :] = near * reach - far * slope
        for p in range(GROUP):
            z = base + p
            weights = plane_weights(fraction_ref, table_ref, view, z)
            start = 1 - shift_ref[view, z]
            for f in range(2):
                grad = resampled(gbuf, (p, f), start, -1, weights, lane)
                for h in range(2):
                    rows = pl.ds(HALF * h, HALF)
                    first = [pair[f][z, rows, :] for pair in old]
                    value = fields[f][z, rows, :] - adam_change(view, grad[h], first)
                    fbuf[p, f, pl.ds(TOP + HALF * h, HALF), :] = value
                    if not last:
                        new_fields[f][z, rows, :] = value
                        grads[f][z, rows, :] = grad[h]
        if last:
            for f in range(2):
                for g in range(GROUP // HALF):
                    for h in range(2):
                        block = fbuf[pl.ds(g * HALF, HALF), f, pl.ds(TOP + HALF * h, HALF), :]
                        sent_ref[pl.ds(HALF * h, HALF), pl.ds(f * depth_planes + base + g * HALF, HALF), :] = (
                            jnp.transpose(block, (1, 0, 2)))
            return carry
        return forward_group(view + 1, base, fbuf, list(carry), (shift_ref, fraction_ref, table_ref),
                             new_kept, lane, planes)

    if last:
        lax.fori_loop(0, depth_planes // GROUP, step, 0)
    else:
        put_slab(slab_ref, lax.fori_loop(0, depth_planes // GROUP, step, fresh_carry()))


def pack_kernel(e_ref, a_ref, goal_ref, shift_ref, fraction_ref, table_ref,
                sent_ref, shift_out, fraction_out, table_out,
                e_buf, a_buf, goal_buf, sems, small_sems):
    depth_planes = e_ref.shape[0]
    span = depth_planes // CHUNKS
    copies = [
        [pltpu.make_async_copy(ref.at[pl.ds(c * span, span)], buf.at[pl.ds(c * span, span)], sems.at[f, c])
         for c in range(CHUNKS)]
        for f, (ref, buf) in enumerate(((e_ref, e_buf), (a_ref, a_buf)))
    ]
    small = [
        pltpu.make_async_copy(ref, buf, small_sems.at[n])
        for n, (ref, buf) in enumerate((
            (goal_ref, goal_buf), (shift_ref, shift_out), (fraction_ref, fraction_out), (table_ref, table_out)))
    ]
    for c in [*copies[0], *copies[1], *small]:
        c.start()
    for f, buf in enumerate((e_buf, a_buf)):
        for c in range(CHUNKS):
            copies[f][c].wait()
            for g in range(span // HALF):
                z = c * span + g * HALF
                for h in range(2):
                    rows = pl.ds(HALF * h, HALF)
                    sent_ref[rows, pl.ds(f * depth_planes + z, HALF), :] = jnp.transpose(
                        buf[pl.ds(z, HALF), rows, :], (1, 0, 2))
    for c in small:
        c.wait()
    for t in range(goal_ref.shape[1]):
        sent_ref[t, pl.ds(2 * depth_planes, ITERS), :] = goal_buf[:, t, :]


def unpack_kernel(sent_ref, e_ref, a_ref, e_buf, a_buf, sems):
    depth_planes = e_ref.shape[0]
    span = depth_planes // CHUNKS
    copies = []
    for f, (ref, buf) in enumerate(((e_ref, e_buf), (a_ref, a_buf))):
        for c in range(CHUNKS):
            for g in range(span // HALF):
                z = c * span + g * HALF
                for h in range(2):
                    rows = pl.ds(HALF * h, HALF)
                    buf[pl.ds(z, HALF), rows, :] = jnp.transpose(
                        sent_ref[rows, pl.ds(f * depth_planes + z, HALF), :], (1, 0, 2))
            copy = pltpu.make_async_copy(
                buf.at[pl.ds(c * span, span)], ref.at[pl.ds(c * span, span)], sems.at[f, c])
            copy.start()
            copies.append(copy)
    for copy in copies:
        copy.wait()


HBM = pl.BlockSpec(memory_space=pltpu.HBM)
VMEM = pl.BlockSpec(memory_space=pltpu.VMEM)
SMEM = pl.BlockSpec(memory_space=pltpu.SMEM)


def call(kernel, in_specs, out_specs, out_shape, scratch, name):
    return pl.pallas_call(
        kernel,
        in_specs=in_specs,
        out_specs=out_specs,
        out_shape=out_shape,
        scratch_shapes=scratch,
        interpret=INTERPRET,
        name=name,
        compiler_params=pltpu.CompilerParams(vmem_limit_bytes=16 * 1024 * 1024),
    )


def body(emission, absorption, target, shift_whole, shift_fraction, taps_table):
    depth_planes, tiles, width = emission.shape
    slabs = lax.axis_size("depth")
    planes = depth_planes * slabs
    volume = jax.ShapeDtypeStruct(emission.shape, jnp.float32)
    slab = jax.ShapeDtypeStruct((slabs, 2, tiles, width), jnp.float32)
    goals = jax.ShapeDtypeStruct((ITERS, tiles, width), jnp.float32)
    padded = pltpu.VMEM((GROUP, 2, PADDED, width), jnp.float32)
    store = pltpu.VMEM(emission.shape, jnp.float32)
    sems = pltpu.SemaphoreType.DMA((2, CHUNKS))

    raw = [
        pltpu.with_memory_space_constraint(x, pltpu.HBM)
        for x in (emission, absorption, target, shift_whole, shift_fraction, taps_table.T)
    ]
    packed, *scalars = call(
        pack_kernel, [HBM] * 6, [VMEM] * 4,
        [jax.ShapeDtypeStruct((tiles, 2 * depth_planes + HALF, width), jnp.float32)]
        + [jax.ShapeDtypeStruct(x.shape, x.dtype) for x in raw[3:]],
        [store, store, pltpu.VMEM(target.shape, jnp.float32), sems, pltpu.SemaphoreType.DMA((4,))], "pack",
    )(*raw)
    packed = lax.all_to_all(packed, "lat", 0, 0, tiled=True)
    e, a, goal, *kept, sums = call(
        functools.partial(first_kernel, planes), [SMEM] * 3 + [VMEM], [VMEM] * 7,
        [volume, volume, goals, volume, volume, volume, slab], [padded], "first",
    )(*scalars, packed)
    old = []
    for view in range(ITERS):
        everyone = lax.all_to_all(sums, "depth", 0, 0, tiled=True)
        operands = (*scalars, everyone, goal, e, a, *old, *kept)
        in_specs = [SMEM] * 3 + [VMEM] * (len(operands) - 3)
        kernel = functools.partial(later_kernel, view, planes)
        if view == ITERS - 1:
            packed = call(
                kernel, in_specs, VMEM,
                jax.ShapeDtypeStruct((tiles, 2 * depth_planes, width), jnp.float32), [padded, padded], "last",
            )(*operands)
        else:
            e, a, g_e, g_a, *kept, sums = call(
                kernel, in_specs, [VMEM] * 8, [volume] * 7 + [slab], [padded, padded], "middle",
            )(*operands)
            old = [*old, g_e, g_a]
    packed = lax.all_to_all(packed, "lat", 0, 0, tiled=True)
    return call(
        unpack_kernel, [VMEM], [HBM, HBM], [volume, volume], [store, store, sems], "unpack")(packed)


def solution(mesh):
    in_specs = (
        P("depth", None, "lat"),
        P("depth", None, "lat"),
        P(None, None, "lat"),
        P(None, "depth"),
        P(None, "depth"),
        P(),
    )
    out_specs = (P("depth", None, "lat"), P("depth", None, "lat"))
    return jax.shard_map(body, mesh=mesh, in_specs=in_specs, out_specs=out_specs, check_vma=False)
```

```python
import functools
import math

import jax
import jax.numpy as jnp
from jax import lax
from jax.experimental import pallas as pl
from jax.experimental.pallas import tpu as pltpu
from jax.sharding import PartitionSpec as P

ITERS = 3
LEARN_RATE = 0.1
BETA_FIRST = 0.9
BETA_SECOND = 0.999
ADAM_EPSILON = 0.001
LOG2E = 1.4426950408889634
TINY = 1e-37

LANES = 128
HALF = 8
TOP = 8
PADDED = 32
GROUP = 64
CHUNKS = 4
INTERPRET = False


def halves(ref, *lead):
    return [ref[(*lead, pl.ds(HALF * h, HALF), slice(None))] for h in range(2)]


def put_halves(ref, lead, values):
    for h in range(2):
        ref[(*lead, pl.ds(HALF * h, HALF), slice(None))] = values[h]


def resampled(buf, lead, start, step, weights, lane):
    total = [None, None]
    for k, weight in enumerate(weights):
        lag = start + step * k
        behind = lag >> 31
        wrapped = lane < (lag & (LANES - 1))
        turn = (-lag) & (LANES - 1)
        for h in range(2):
            here = buf[(*lead, pl.ds(behind + (TOP + HALF * h), HALF), slice(None))]
            after = buf[(*lead, pl.ds(behind + (TOP + HALF * h + 1), HALF), slice(None))]
            term = weight * pltpu.roll(jnp.where(wrapped, after, here), turn, 1)
            total[h] = term if total[h] is None else total[h] + term
    return total


def plane_weights(fraction_ref, table_ref, view, z):
    column = fraction_ref[view, z]
    return [table_ref[k, column] for k in range(table_ref.shape[0])]


def adam_change(view, grad, first):
    power = view + 1
    if view == 0:
        return LEARN_RATE * grad / (jnp.abs(grad) + ADAM_EPSILON), (grad,)
    old_top, old_square = (first[0], first[0] * first[0]) if view == 1 else first
    top = BETA_FIRST * old_top + grad
    square = BETA_SECOND * old_square + grad * grad
    scale = math.sqrt((1.0 - BETA_SECOND) / (1.0 - BETA_SECOND**power))
    rate = LEARN_RATE * (1.0 - BETA_FIRST) / (1.0 - BETA_FIRST**power) / scale
    root = square * lax.rsqrt(jnp.maximum(square, TINY))
    return rate * top / (root + ADAM_EPSILON / scale), (top, square)


def march(color, density, carry, planes):
    passing, light = carry
    density = density * LOG2E
    fade = jnp.exp2(-jnp.abs(density))
    soft = jnp.maximum(density, 0.0) + jnp.log2(1.0 + fade)
    slope = jnp.exp2(density - soft)
    unit = 1.0 / (planes * LOG2E)
    opacity = soft * (unit - soft * (unit**2 / 2.0 - soft * (unit**3 / 6.0)))
    blend = passing * opacity
    passing = passing - blend
    light = light + blend * color
    reach = slope * (passing * color + light)
    return (passing, light), (blend, reach, slope)


def clear_edges(buf):
    blank = jnp.zeros((HALF, LANES), jnp.float32)
    for p in range(buf.shape[0]):
        for f in range(buf.shape[1]):
            buf[p, f, pl.ds(0, TOP), :] = blank
            buf[p, f, pl.ds(TOP + 2 * HALF, HALF), :] = blank


def lane_index():
    return lax.broadcasted_iota(jnp.int32, (HALF, LANES), 1)


def fresh_carry():
    zero = jnp.zeros((HALF, LANES), jnp.float32)
    return [(zero + 1.0, zero) for _ in range(2)]


def forward_group(view, base, buf, carry, scalars, outs, lane, planes):
    shift_ref, fraction_ref, table_ref = scalars
    for p in range(GROUP):
        z = base + p
        weights = plane_weights(fraction_ref, table_ref, view, z)
        start = shift_ref[view, z] - 1
        color = resampled(buf, (p, 0), start, 1, weights, lane)
        density = resampled(buf, (p, 1), start, 1, weights, lane)
        for h in range(2):
            carry[h], kept = march(color[h], density[h], carry[h], planes)
            for ref, value in zip(outs, kept):
                ref[z, pl.ds(HALF * h, HALF), :] = value
    return carry


def put_slab(slab_ref, carry):
    for i in range(slab_ref.shape[0]):
        put_halves(slab_ref, (i, 0), [carry[h][1] for h in range(2)])
        put_halves(slab_ref, (i, 1), [carry[h][0] for h in range(2)])


def first_kernel(planes, shift_ref, fraction_ref, table_ref, sent_ref, e_ref, a_ref, goal_ref,
                 blend_ref, reach_ref, slope_ref, slab_ref, buf):
    depth_planes = e_ref.shape[0]
    clear_edges(buf)
    lane = lane_index()
    for t in range(goal_ref.shape[1]):
        goal_ref[:, t, :] = sent_ref[t, pl.ds(2 * depth_planes, ITERS), :]

    def step(i, carry):
        base = pl.multiple_of(i * GROUP, GROUP)
        for f, ref in enumerate((e_ref, a_ref)):
            for g in range(GROUP // HALF):
                for h in range(2):
                    rows = pl.ds(HALF * h, HALF)
                    block = jnp.transpose(
                        sent_ref[rows, pl.ds(f * depth_planes + base + g * HALF, HALF), :], (1, 0, 2))
                    ref[pl.ds(base + g * HALF, HALF), rows, :] = block
                    buf[pl.ds(g * HALF, HALF), f, pl.ds(TOP + HALF * h, HALF), :] = block
        return forward_group(0, base, buf, list(carry), (shift_ref, fraction_ref, table_ref),
                             (blend_ref, reach_ref, slope_ref), lane, planes)

    put_slab(slab_ref, lax.fori_loop(0, depth_planes // GROUP, step, fresh_carry()))


def combined_rays(view, slabs_ref, goal_ref, planes):
    here = lax.axis_index("depth")
    found = []
    for h in range(2):
        rows = pl.ds(HALF * h, HALF)
        image = jnp.zeros((HALF, LANES), jnp.float32)
        front = image
        passing = image + 1.0
        clear = passing
        for i in range(slabs_ref.shape[0]):
            front = jnp.where(here == i, image, front)
            clear = jnp.where(here == i, passing, clear)
            image = image + passing * slabs_ref[i, 0, rows, :]
            passing = passing * slabs_ref[i, 1, rows, :]
        residual = image - goal_ref[view, rows, :]
        near = residual * clear
        found.append((near * planes, near, residual * (image - front)))
    return found


def later_kernel(view, planes, *refs):
    last = view == ITERS - 1
    refs = list(refs)

    def take(n):
        taken = refs[:n]
        del refs[:n]
        return taken

    shift_ref, fraction_ref, table_ref, slabs_ref, goal_ref = take(5)
    fields = take(2)
    old = [take(2) for _ in range(view)]
    kept = take(3)
    if last:
        (sent_ref,) = take(1)
        gbuf, fbuf = refs
    else:
        new_fields, states, new_kept, (slab_ref,) = take(2), [take(2) for _ in range(view + 1)], take(3), take(1)
        gbuf, fbuf = refs
        clear_edges(fbuf)
    clear_edges(gbuf)
    lane = lane_index()
    rays = combined_rays(view, slabs_ref, goal_ref, planes)
    depth_planes = fields[0].shape[0]

    def step(i, carry):
        base = pl.multiple_of(i * GROUP, GROUP)
        for p in range(GROUP):
            for h in range(2):
                rows = pl.ds(HALF * h, HALF)
                blend, reach, slope = (ref[base + p, rows, :] for ref in kept)
                scaled, near, far = rays[h]
                gbuf[p, 0, pl.ds(TOP + HALF * h, HALF), :] = scaled * blend
                gbuf[p, 1, pl.ds(TOP + HALF * h, HALF), :] = near * reach - far * slope
        for p in range(GROUP):
            z = base + p
            weights = plane_weights(fraction_ref, table_ref, view, z)
            start = 1 - shift_ref[view, z]
            for f in range(2):
                grad = resampled(gbuf, (p, f), start, -1, weights, lane)
                for h in range(2):
                    rows = pl.ds(HALF * h, HALF)
                    first = [pair[f][z, rows, :] for pair in old]
                    change, state = adam_change(view, grad[h], first)
                    value = fields[f][z, rows, :] - change
                    fbuf[p, f, pl.ds(TOP + HALF * h, HALF), :] = value
                    if not last:
                        new_fields[f][z, rows, :] = value
                        for pair, moment in zip(states, state):
                            pair[f][z, rows, :] = moment
        if last:
            for f in range(2):
                for g in range(GROUP // HALF):
                    for h in range(2):
                        block = fbuf[pl.ds(g * HALF, HALF), f, pl.ds(TOP + HALF * h, HALF), :]
                        sent_ref[pl.ds(HALF * h, HALF), pl.ds(f * depth_planes + base + g * HALF, HALF), :] = (
                            jnp.transpose(block, (1, 0, 2)))
            return carry
        return forward_group(view + 1, base, fbuf, list(carry), (shift_ref, fraction_ref, table_ref),
                             new_kept, lane, planes)

    if last:
        lax.fori_loop(0, depth_planes // GROUP, step, 0)
    else:
        put_slab(slab_ref, lax.fori_loop(0, depth_planes // GROUP, step, fresh_carry()))


def pack_kernel(e_ref, a_ref, goal_ref, shift_ref, fraction_ref, table_ref,
                sent_ref, shift_out, fraction_out, table_out,
                e_buf, a_buf, goal_buf, sems, small_sems):
    depth_planes = e_ref.shape[0]
    span = depth_planes // CHUNKS
    copies = [
        [pltpu.make_async_copy(ref.at[pl.ds(c * span, span)], buf.at[pl.ds(c * span, span)], sems.at[f, c])
         for c in range(CHUNKS)]
        for f, (ref, buf) in enumerate(((e_ref, e_buf), (a_ref, a_buf)))
    ]
    small = [
        pltpu.make_async_copy(ref, buf, small_sems.at[n])
        for n, (ref, buf) in enumerate((
            (goal_ref, goal_buf), (shift_ref, shift_out), (fraction_ref, fraction_out), (table_ref, table_out)))
    ]
    for c in [*copies[0], *copies[1], *small]:
        c.start()
    for f, buf in enumerate((e_buf, a_buf)):
        for c in range(CHUNKS):
            copies[f][c].wait()
            for g in range(span // HALF):
                z = c * span + g * HALF
                for h in range(2):
                    rows = pl.ds(HALF * h, HALF)
                    sent_ref[rows, pl.ds(f * depth_planes + z, HALF), :] = jnp.transpose(
                        buf[pl.ds(z, HALF), rows, :], (1, 0, 2))
    for c in small:
        c.wait()
    for t in range(goal_ref.shape[1]):
        sent_ref[t, pl.ds(2 * depth_planes, ITERS), :] = goal_buf[:, t, :]


def unpack_kernel(sent_ref, e_ref, a_ref, e_buf, a_buf, sems):
    depth_planes = e_ref.shape[0]
    span = depth_planes // CHUNKS
    copies = []
    for f, (ref, buf) in enumerate(((e_ref, e_buf), (a_ref, a_buf))):
        for c in range(CHUNKS):
            for g in range(span // HALF):
                z = c * span + g * HALF
                for h in range(2):
                    rows = pl.ds(HALF * h, HALF)
                    buf[pl.ds(z, HALF), rows, :] = jnp.transpose(
                        sent_ref[rows, pl.ds(f * depth_planes + z, HALF), :], (1, 0, 2))
            copy = pltpu.make_async_copy(
                buf.at[pl.ds(c * span, span)], ref.at[pl.ds(c * span, span)], sems.at[f, c])
            copy.start()
            copies.append(copy)
    for copy in copies:
        copy.wait()


HBM = pl.BlockSpec(memory_space=pltpu.HBM)
VMEM = pl.BlockSpec(memory_space=pltpu.VMEM)
SMEM = pl.BlockSpec(memory_space=pltpu.SMEM)


def call(kernel, in_specs, out_specs, out_shape, scratch, name):
    return pl.pallas_call(
        kernel,
        in_specs=in_specs,
        out_specs=out_specs,
        out_shape=out_shape,
        scratch_shapes=scratch,
        interpret=INTERPRET,
        name=name,
        compiler_params=pltpu.CompilerParams(vmem_limit_bytes=16 * 1024 * 1024),
    )


def body(emission, absorption, target, shift_whole, shift_fraction, taps_table):
    depth_planes, tiles, width = emission.shape
    slabs = lax.axis_size("depth")
    planes = depth_planes * slabs
    volume = jax.ShapeDtypeStruct(emission.shape, jnp.float32)
    slab = jax.ShapeDtypeStruct((slabs, 2, tiles, width), jnp.float32)
    goals = jax.ShapeDtypeStruct((ITERS, tiles, width), jnp.float32)
    padded = pltpu.VMEM((GROUP, 2, PADDED, width), jnp.float32)
    store = pltpu.VMEM(emission.shape, jnp.float32)
    sems = pltpu.SemaphoreType.DMA((2, CHUNKS))

    raw = [
        pltpu.with_memory_space_constraint(x, pltpu.HBM)
        for x in (emission, absorption, target, shift_whole, shift_fraction, taps_table.T)
    ]
    packed, *scalars = call(
        pack_kernel, [HBM] * 6, [VMEM] * 4,
        [jax.ShapeDtypeStruct((tiles, 2 * depth_planes + HALF, width), jnp.float32)]
        + [jax.ShapeDtypeStruct(x.shape, x.dtype) for x in raw[3:]],
        [store, store, pltpu.VMEM(target.shape, jnp.float32), sems, pltpu.SemaphoreType.DMA((4,))], "pack",
    )(*raw)
    packed = lax.all_to_all(packed, "lat", 0, 0, tiled=True)
    e, a, goal, *kept, sums = call(
        functools.partial(first_kernel, planes), [SMEM] * 3 + [VMEM], [VMEM] * 7,
        [volume, volume, goals, volume, volume, volume, slab], [padded], "first",
    )(*scalars, packed)
    old = []
    for view in range(ITERS):
        everyone = lax.all_to_all(sums, "depth", 0, 0, tiled=True)
        operands = (*scalars, everyone, goal, e, a, *old, *kept)
        in_specs = [SMEM] * 3 + [VMEM] * (len(operands) - 3)
        kernel = functools.partial(later_kernel, view, planes)
        if view == ITERS - 1:
            packed = call(
                kernel, in_specs, VMEM,
                jax.ShapeDtypeStruct((tiles, 2 * depth_planes, width), jnp.float32), [padded, padded], "last",
            )(*operands)
        else:
            moments = 2 * (view + 1)
            e, a, *rest, sums = call(
                kernel, in_specs, [VMEM] * (moments + 6), [volume] * (moments + 5) + [slab],
                [padded, padded], "middle",
            )(*operands)
            old, kept = rest[:moments], rest[moments:]
    packed = lax.all_to_all(packed, "lat", 0, 0, tiled=True)
    return call(
        unpack_kernel, [VMEM], [HBM, HBM], [volume, volume], [store, store, sems], "unpack")(packed)


def solution(mesh):
    in_specs = (
        P("depth", None, "lat"),
        P("depth", None, "lat"),
        P(None, None, "lat"),
        P(None, "depth"),
        P(None, "depth"),
        P(),
    )
    out_specs = (P("depth", None, "lat"), P("depth", None, "lat"))
    return jax.shard_map(body, mesh=mesh, in_specs=in_specs, out_specs=out_specs, check_vma=False)
```
